32 devices in a mesh: dp: 8 (over y, x, core), tensor: 4 (over z).
Axes of the slice: x: 2, y: 2, z: 4, core: 2. Of those that a mesh axis runs over, the one named last changes fastest.
Arguments:
- memory: bfloat16 [12288, 1280], P('dp'), may hold values from -6 to 6
- hidden: bfloat16 [12288, 2560], P('dp', 'tensor'), may hold values from -6 to 6
- grad_out: bfloat16 [12288, 2560], P('dp', 'tensor'), may hold values from -6 to 6
- key_weight: bfloat16 [1280, 2560], P('dp', 'tensor'), may hold values from -0.15625 to 0.15625
- value_weight: bfloat16 [1280, 2560], P('dp', 'tensor'), may hold values from -0.15625 to 0.15625
- row_ids: int32 [12288, 5], P('dp'), may hold values from 0 to 65535, as said below
- embed_table: float32 [65536, 256], P(('dp', 'tensor')), may hold values from -6 to 6
- first_moment: float32 [65536, 256], P(('dp', 'tensor')), may hold values from -0.6 to 0.6
- second_moment: float32 [65536, 256], P(('dp', 'tensor')), may hold values from 0.001 to 0.1
Outputs:
- key_weight_grad: float32 [1280, 2560], P('dp', 'tensor')
- value_weight_grad: float32 [1280, 2560], P('dp', 'tensor')
- new_table: float32 [65536, 256], P(('dp', 'tensor'))
- new_first: float32 [65536, 256], P(('dp', 'tensor'))
- new_second: float32 [65536, 256], P(('dp', 'tensor'))
The draws below stay inside these ranges and needn't reach their ends.
Inputs may be any that keep to these rules, and one draw needn't show every extreme that they name: `row_ids`: the table's rows fall into 32 owners of 2048 consecutive rows each. Taking the tokens in aligned blocks of 384 consecutive tokens with all their 5 ids, at most 180 ids of one block fall in one owner's rows, and in every block some owner gets exactly 180 of them.
All inputs are finite; a program needn't handle non-finite values.
Results may differ from the reference program's by a relative error of at most 0.0043.
Values may be sent and summed in bfloat16 or wider, within the bound.
A program may use at most 128 MiB of HBM per device.

```python
import math
import jax
import jax.numpy as jnp
from jax import lax

D = 2560
ROW_W = 256
LOOKUPS = 5
MEM = 1280
ROWS_DEV = 2048
BLOCK = 384
CAP = 180
TOKENS = 12288
ROWS = 65536
DEVICES = 32


def block_ids(block_key):
    entries = BLOCK * LOOKUPS
    owners = DEVICES
    slots = owners * CAP
    keys = jax.random.split(block_key, 5)
    loads = jax.random.randint(keys[0], (owners,), 1, CAP + 1)
    hottest = jax.random.randint(keys[1], (), 0, owners)
    slot_index = jnp.arange(slots, dtype=jnp.int32)
    slot_owner = slot_index // CAP
    slot_copy = slot_index % CAP
    tier = jnp.where(slot_owner == hottest, 2, jnp.where(slot_copy < loads[slot_owner], 1, 0))
    noise = jax.random.randint(keys[2], (slots,), 0, 2048)
    score = tier * 16777216 + noise * 8192 + slot_index
    chosen = lax.top_k(score, entries)[1]
    owner_of = jax.random.permutation(keys[3], chosen // CAP)
    local_row = jax.random.randint(keys[4], (entries,), 0, ROWS_DEV)
    return (owner_of * ROWS_DEV + local_row).astype(jnp.int32)


def draw_row_ids(key, part):
    count = TOKENS // BLOCK
    keys = jax.random.split(jax.random.fold_in(key, 7), count)
    table_ids = jax.vmap(block_ids)(keys)
    return table_ids.reshape(TOKENS, LOOKUPS).astype(jnp.int32)


def block_levels(own_key, extent, cuts, low, top_value):
    factor_of = 1.0
    for position, blocks in cuts:
        steps = jax.random.uniform(jax.random.fold_in(jax.random.fold_in(own_key, 6), position), (blocks,), jnp.float32, low / len(cuts), top_value / len(cuts))
        factor_of = factor_of * jnp.repeat(jnp.exp(steps), extent[position] // blocks).reshape((-1,) + (1,) * (len(extent) - 1 - position))
    return factor_of


def normal_values(rng, dims, spread, reach, shards=(), kind=jnp.bfloat16):
    values = spread * jax.random.normal(rng, dims, jnp.float32)
    if shards:
        values = values * block_levels(rng, dims, shards, -0.22, 0.18)
    return jnp.clip(values, -reach, reach).astype(kind)


def setup_inputs(seed: int = 0) -> dict:
    streams_of = jax.random.split(jax.random.key(seed), 10)
    return {
        "memory": normal_values(streams_of[0], (TOKENS, MEM), 1.0, 6.0, ((0, 8),)),
        "hidden": normal_values(streams_of[1], (TOKENS, D), 1.0, 6.0, ((0, 8), (1, 4))),
        "grad_out": normal_values(streams_of[2], (TOKENS, D), 1.0, 6.0, ((0, 8), (1, 4))),
        "key_weight": normal_values(streams_of[3], (MEM, D), MEM ** -0.5, 0.15625, ((0, 8), (1, 4))),
        "value_weight": normal_values(streams_of[4], (MEM, D), MEM ** -0.5, 0.15625, ((0, 8), (1, 4))),
        "row_ids": draw_row_ids(jax.random.fold_in(streams_of[9], 71), 0),
        "embed_table": normal_values(streams_of[6], (ROWS, ROW_W), 1.0, 6.0, ((0, 32),), jnp.float32),
        "first_moment": normal_values(streams_of[7], (ROWS, ROW_W), 0.1, 0.6, ((0, 32),), jnp.float32),
        "second_moment": jnp.clip(jnp.exp(math.log(0.1) - 4.6051702 * jax.random.uniform(streams_of[8], (ROWS, ROW_W), jnp.float32) ** block_levels(streams_of[8], (ROWS, ROW_W), ((0, 32),), -0.2, 0.2)), 0.001, 0.1),
    }


beta_one = 0.9
beta_two = 0.999
learn_rate = 0.01
adam_eps = 1e-08
norm_eps = 1e-06
correct_one = 0.9999734386011124
correct_two = 0.0952078528863

def adam_update(table_grad, embed_table, first_moment, second_moment):
    new_first = beta_one * first_moment + (1.0 - beta_one) * table_grad
    new_second = beta_two * second_moment + (1.0 - beta_two) * table_grad * table_grad
    stepped = new_first / correct_one / (jnp.sqrt(new_second / correct_two) + adam_eps)
    return (embed_table - learn_rate * stepped, new_first, new_second)

def reference(memory, hidden, grad_out, key_weight, value_weight, row_ids, embed_table, first_moment, second_moment):
    key_proj = jnp.dot(memory, key_weight, preferred_element_type=jnp.float32)
    value_proj = jnp.dot(memory, value_weight, preferred_element_type=jnp.float32)
    hidden_float = hidden.astype(jnp.float32)
    grad_float = grad_out.astype(jnp.float32)
    root_width = math.sqrt(D)
    key_scale = jnp.sqrt(lax.optimization_barrier(jnp.mean(key_proj * key_proj, axis=1, keepdims=True)) + norm_eps)
    gate_score = lax.optimization_barrier(jnp.sum(hidden_float * key_proj, axis=1, keepdims=True)) / (key_scale * root_width)
    gate_value = jax.nn.sigmoid(gate_score)
    gate_grad = gate_value * (1.0 - gate_value) * lax.optimization_barrier(jnp.sum(grad_float * value_proj, axis=1, keepdims=True))
    value_grad = (gate_value * grad_float).astype(jnp.bfloat16)
    key_grad = (gate_grad * (hidden_float / (key_scale * root_width) - gate_score * key_proj / (D * key_scale * key_scale))).astype(jnp.bfloat16)
    contract = (((0,), (0,)), ((), ()))
    key_weight_grad = lax.dot_general(memory, key_grad, contract, preferred_element_type=jnp.float32)
    value_weight_grad = lax.dot_general(memory, value_grad, contract, preferred_element_type=jnp.float32)
    memory_grad = jnp.dot(key_grad, key_weight.T, preferred_element_type=jnp.float32) + jnp.dot(value_grad, value_weight.T, preferred_element_type=jnp.float32)
    memory_grad = memory_grad.astype(jnp.bfloat16)
    pieces = memory_grad.reshape(-1, ROW_W).astype(jnp.float32)
    table_grad = jnp.zeros(embed_table.shape, jnp.float32).at[row_ids.reshape(-1).astype(jnp.int32)].add(pieces)
    new_table, new_first, new_second = adam_update(table_grad, embed_table, first_moment, second_moment)
    return (key_weight_grad, value_weight_grad, new_table, new_first, new_second)
```

```python
import math

import jax
import jax.numpy as jnp
from jax import lax
from jax.experimental import pallas as pl
from jax.experimental.pallas import tpu as pltpu
from jax.sharding import PartitionSpec as P

beta_one = 0.9
beta_two = 0.999
learn_rate = 0.01
adam_eps = 1e-08
norm_eps = 1e-06
correct_one = 0.9999734386011124
correct_two = 0.0952078528863


f32 = jnp.float32
bf16 = jnp.bfloat16
lanes = 128
sublanes = 8


MESH = pl.DeviceIdType.MESH
contract_lanes = (((1,), (1,)), ((), ()))
contract_rows = (((0,), (0,)), ((), ()))


def divisor(count, choices):
    return next((c for c in choices if count % c == 0), count)


def step_kernel(
    plan,
    memory_hbm,
    hidden_hbm,
    grad_hbm,
    key_w_hbm,
    value_w_hbm,
    ids_hbm,
    key_out,
    value_out,
    table_out,
    mem_s,
    hid_s,
    grd_s,
    w_s,
    w_slab_s,
    key_s,
    both_s,
    part_s,
    in_s,
    mid_s,
    total_s,
    sums_s,
    ids_s,
    slot_s,
    own_s,
    gid_s,
    send_s,
    got_s,
    wg_s,
    wg_slab_s,
    pair_s,
    half_s,
    local_sem,
    ids_ssem,
    ids_rsem,
    ag_ssem,
    ag_rsem,
    dd_ssem,
    dd_rsem,
    sum_ssem,
    sum_rsem,
    part_ssem,
    part_rsem,
    mid_ssem,
    mid_rsem,
    total_ssem,
    total_rsem,
    row_ssem,
    row_rsem,
    pair_ssem,
    pair_rsem,
    half_ssem,
    half_rsem,
):
    dp_count, t_count = plan["dp"], plan["tensor"]
    tokens, mem, width = plan["tokens"], plan["mem"], plan["width"]
    shard, cap, rows_dev = plan["shard"], plan["cap"], plan["rows_dev"]
    lookups, row_width = plan["lookups"], plan["row_width"]
    blocks, block, tile, chunk = t_count, plan["block"], plan["tile"], plan["chunk"]
    aligned = plan["aligned"]
    model_width = width * t_count
    entries = block * lookups
    chips = dp_count // 2
    bits = chips.bit_length() - 1
    chunks = tokens // chunk
    tiles = tokens // tile
    per_tile = tile // chunk
    wide = plan["wide"]
    wides = tokens // wide
    per_wide = wide // tile
    per_block = block // chunk
    slots = dp_count * cap

    me = lax.axis_index("dp")
    z = lax.axis_index("tensor")
    core = me % 2
    chip = me // 2
    partner = chip * 2 + 1 - core
    is_mid = jnp.logical_and(z > 0, z < t_count - 1)
    is_end = jnp.logical_or(z == 0, z == t_count - 1)
    mate = z + 1 - 2 * (z % 2)
    other = t_count - 1 - z

    def remote(src, dst, ssem, rsem, dev_dp, dev_z):
        return pltpu.make_async_remote_copy(
            src_ref=src,
            dst_ref=dst,
            send_sem=ssem,
            recv_sem=rsem,
            device_id=(dev_dp, dev_z),
            device_id_type=MESH,
        )

    def slab_of(flat, stacked, index):
        if aligned:
            return flat.at[pl.ds(pl.multiple_of(index * shard, shard), shard)]
        return stacked.at[index]

    def w_slab(index):
        return slab_of(w_s, w_slab_s, index)

    def wg_slab(index):
        return slab_of(wg_s, wg_slab_s, index)

    own = w_slab(me)
    local = [
        pltpu.make_async_copy(key_w_hbm, own.at[:, :width], local_sem.at[0]),
        pltpu.make_async_copy(value_w_hbm, own.at[:, width:], local_sem.at[1]),
        pltpu.make_async_copy(ids_hbm, ids_s.at[me], local_sem.at[2]),
        pltpu.make_async_copy(memory_hbm, mem_s, local_sem.at[3]),
        pltpu.make_async_copy(hidden_hbm, hid_s, local_sem.at[4]),
        pltpu.make_async_copy(grad_hbm, grd_s, local_sem.at[5]),
    ]
    for copy in local:
        copy.start()

    barrier = pltpu.get_barrier_semaphore()
    for i in range(1, dp_count):
        pl.semaphore_signal(
            barrier, inc=1, device_id=((me + i) % dp_count, z), device_id_type=MESH
        )
    for i in range(1, t_count):
        pl.semaphore_signal(
            barrier, inc=1, device_id=(me, (z + i) % t_count), device_id_type=MESH
        )
    pl.semaphore_wait(barrier, dp_count - 1 + t_count - 1)

    def flip(x, s):
        a, b = 1 << s, 1 << (bits - 1 - s)
        f0 = x + a * (1 - 2 * ((x // a) % 2))
        f1 = x + b * (1 - 2 * ((x // b) % 2))
        return f0 * (1 - core) + f1 * core

    have = [chip]
    for s in range(bits):
        have = have + [flip(x, s) for x in have]

    def gather_copy(s, k):
        at = (1 << s) + k
        ref = w_slab(have[k] * 2 + core)
        return remote(ref, ref, ag_ssem.at[at], ag_rsem.at[at], flip(chip, s) * 2 + core, z)

    def across_copy(k):
        ref = w_slab(have[k] * 2 + core)
        return remote(ref, ref, dd_ssem.at[k], dd_rsem.at[k], partner, z)

    def ids_copy(i):
        ref = ids_s.at[me]
        return remote(ref, ref, ids_ssem.at[i], ids_rsem.at[i], (me + i) % dp_count, z)

    local[0].wait()
    local[1].wait()
    across_copy(0).start()
    for s in range(bits):
        if s:
            gather_copy(s - 1, 0).wait_send()
        gather_copy(s, 0).start()
    local[2].wait()

    upper = (
        lax.broadcasted_iota(jnp.int32, (lanes, lanes), 0)
        <= lax.broadcasted_iota(jnp.int32, (lanes, lanes), 1)
    )
    upper = jnp.where(upper, 1.0, 0.0).astype(bf16)

    def running(hits):
        carry = jnp.zeros((hits.shape[0], 1), f32)
        parts = []
        for start in range(0, entries, lanes):
            part = carry + jnp.dot(
                hits[:, start : start + lanes].astype(bf16), upper, preferred_element_type=f32
            )
            carry = part[:, lanes - 1 : lanes]
            parts.append(part)
        return jnp.concatenate(parts, axis=1)

    dest = lax.broadcasted_iota(jnp.int32, (dp_count, entries), 0)
    for b in range(blocks):
        owner_of = lax.div(ids_s[me, b : b + 1, :], jnp.int32(rows_dev))
        hits = jnp.where(owner_of == dest * t_count + z, 1.0, 0.0)
        ranked = hits * (running(hits) + (dest * cap).astype(f32))
        slot_s[b : b + 1, :] = jnp.sum(ranked, axis=0, keepdims=True).astype(jnp.int32) - 1

    def forward(k):
        s = k.bit_length() - 1
        gather_copy(s, k - (1 << s)).wait_recv()
        for later in range(s + 1, bits):
            gather_copy(later, k).start()
        across_copy(k).start()

    for k in range(1, chips):
        forward(k)
    for i in range(1, dp_count):
        ids_copy(i).start()

    def own_slots(j, carry):
        owner_of = lax.div(ids_s[j], jnp.int32(rows_dev))
        hits = jnp.where(owner_of == me * t_count + z, 1.0, 0.0)
        own_s[j] = (hits * running(hits)).astype(jnp.int32) - 1
        return carry

    id_tiles = slots // lanes
    id_parts = divisor(id_tiles, (4, 3, 2))
    id_each = id_tiles // id_parts

    def own_ids(b, part):
        for start in range(part * id_each * lanes, (part + 1) * id_each * lanes, lanes):
            first = start // cap
            last = (start + lanes - 1) // cap
            found = jnp.zeros((sublanes, lanes), f32)
            for j in range(first, last + 1):
                local_row = lax.rem(ids_s[j, pl.ds(b, 1), :], jnp.int32(rows_dev)) + 1
                row = lax.broadcasted_iota(jnp.int32, (sublanes, entries), 0)
                codes = jnp.where(
                    row == 0,
                    lax.div(local_row, jnp.int32(64)),
                    jnp.where(row == 1, lax.rem(local_row, jnp.int32(64)), 0),
                )
                slot = lax.broadcasted_iota(jnp.int32, (lanes, entries), 0) + (start - j * cap)
                hot = jnp.where(slot == own_s[j, pl.ds(b, 1), :], 1.0, 0.0)
                hot = jnp.where(slot < 0, 0.0, hot)
                found = found + lax.dot_general(
                    codes.astype(f32).astype(bf16),
                    hot.astype(bf16),
                    contract_lanes,
                    preferred_element_type=f32,
                )
            ids = found[0:1] * 64.0 + found[1:2] - 1.0
            gid_s[b, :, start : start + lanes] = jnp.broadcast_to(
                ids.astype(jnp.int32), (sublanes, lanes)
            )

    for k in range(chips):
        across_copy(k).wait_recv()
    if not aligned:
        for d in range(dp_count):
            w_s[d * shard : (d + 1) * shard, :] = w_slab_s[d]

    for copy in local[3:]:
        copy.wait()
    def project(i):
        at = pl.ds(pl.multiple_of(i * wide, wide), wide)
        proj = jnp.dot(mem_s[at, :], w_s[...], preferred_element_type=f32)
        key_proj = proj[:, :width]
        key_s[at, :] = key_proj
        square = jnp.sum(key_proj * key_proj, axis=1, keepdims=True)
        cross = jnp.sum(hid_s[at, :].astype(f32) * key_proj, axis=1, keepdims=True)
        output = jnp.sum(grd_s[at, :].astype(f32) * proj[:, width:], axis=1, keepdims=True)
        lane = lax.broadcasted_iota(jnp.int32, (wide, lanes), 1)
        packed = jnp.where(
            lane == 0, square, jnp.where(lane == 1, cross, jnp.where(lane == 2, output, 0.0))
        )
        sums_s[i, z] = packed.T[:sublanes, :]
        for n in range(1, t_count):
            sums_copy(i, n).start()

    def sums_copy(i, n):
        ref = sums_s.at[i, z]
        return remote(ref, ref, sum_ssem.at[i, n], sum_rsem.at[i, n], me, (z + n) % t_count)

    ahead = min(2, wides)
    for i in range(ahead):
        project(i)
    table_out[...] = jnp.zeros(table_out.shape, f32)

    def chunk_at(c):
        return pl.ds(pl.multiple_of(c * chunk, chunk), chunk)

    def part_copy(c):
        at = chunk_at(c)
        return remote(part_s.at[at], in_s.at[at], part_ssem.at[c], part_rsem.at[c], me, mate)

    def mid_copy(c):
        at = chunk_at(c)
        return remote(part_s.at[at], mid_s.at[at], mid_ssem.at[c], mid_rsem.at[c], me, other)

    def total_copy(c):
        at = chunk_at(c)
        return remote(total_s.at[at], total_s.at[at], total_ssem.at[c], total_rsem.at[c], me, mate)

    def grads(i):
        at = pl.ds(pl.multiple_of(i * tile, tile), tile)
        group = i // per_wide

        @pl.when(i % per_wide == 0)
        def _():
            for n in range(1, t_count):
                sums_copy(group, n).wait_recv()

        lane_at = pl.ds(pl.multiple_of((i % per_wide) * tile, tile), tile)
        sums = sums_s[group, 0, :, lane_at]
        for part in range(1, t_count):
            sums = sums + sums_s[group, part, :, lane_at]
        root_width = math.sqrt(model_width)
        key_scale = jnp.sqrt(sums[0:1] / model_width + norm_eps)
        gate_score = sums[1:2] / (key_scale * root_width)
        gate_value = 1.0 / (1.0 + jnp.exp(-gate_score))
        gate_grad = gate_value * (1.0 - gate_value) * sums[2:3]
        hidden_factor = gate_grad / (key_scale * root_width)
        key_factor = gate_grad * (gate_score / (model_width * key_scale * key_scale))
        row = lax.broadcasted_iota(jnp.int32, (lanes, tile), 0)
        factors = jnp.where(
            row == 0, hidden_factor, jnp.where(row == 1, key_factor, gate_value)
        ).T
        both_s[at, :width] = (
            factors[:, 0:1] * hid_s[at, :].astype(f32) - factors[:, 1:2] * key_s[at, :]
        ).astype(bf16)
        both_s[at, width:] = (factors[:, 2:3] * grd_s[at, :].astype(f32)).astype(bf16)
        part_s[at, :] = lax.dot_general(
            both_s[at, :], w_s[...], contract_lanes, preferred_element_type=f32
        ).astype(bf16)

        @pl.when(is_end)
        def _():
            for k in range(per_tile):
                part_copy(i * per_tile + k).start()

    def weight_grad(start, size):
        value = lax.dot_general(
            mem_s[:, start : start + size], both_s[...], contract_rows, preferred_element_type=f32
        ).astype(bf16)
        if aligned:
            wg_s[start : start + size, :] = value
        else:
            at = start
            while at < start + size:
                d = at // shard
                stop = min((d + 1) * shard, start + size)
                wg_slab_s[d, at - d * shard : stop - d * shard, :] = value[
                    at - start : stop - start
                ]
                at = stop

    def pair_copy(k):
        return remote(
            wg_slab(k * 2 + 1 - core), pair_s.at[k], pair_ssem.at[k], pair_rsem.at[k], partner, z
        )

    def half_copy(s, k):
        at = (1 << s) + k
        return remote(
            wg_slab(have[at] * 2 + core),
            half_s.at[at],
            half_ssem.at[at],
            half_rsem.at[at],
            flip(chip, s) * 2 + core,
            z,
        )

    def half_start(s):
        for k in range(1 << s):
            half_copy(s, k).start()

    def pair_sum():
        for k in range(chips):
            pair_copy(k).wait_recv()
        for k in range(chips):
            ref = wg_slab(k * 2 + core)
            ref[...] = (ref[...].astype(f32) + pair_s[k].astype(f32)).astype(bf16)

    def half_sum(s):
        for k in range(1 << s):
            half_copy(s, k).wait_recv()
        for k in range(1 << s):
            ref = wg_slab(have[k] * 2 + core)
            added = ref[...].astype(f32) + half_s[(1 << s) + k].astype(f32)
            if s:
                ref[...] = added.astype(bf16)
            else:
                key_out[...] = added[:, :width]
                value_out[...] = added[:, width:]

    def row_copy(b, j, i):
        return remote(
            send_s.at[b, j], got_s.at[b, me], row_ssem.at[b, i], row_rsem.at[b, i], j, z
        )

    dest_each = dp_count // 4 if dp_count % 4 == 0 else dp_count
    dest_parts = dp_count // dest_each

    def dispatch(b, part):
        def one(i, carry):
            j = (me + i) % dp_count
            slot = lax.broadcasted_iota(jnp.int32, (cap, block), 0) + j * cap
            rows = jnp.zeros((cap, row_width), f32)
            at = pl.ds(pl.multiple_of(b * block, block), block)
            for lookup in range(lookups):
                ids = slot_s[pl.ds(b, 1), lookup * block : (lookup + 1) * block]
                hot = jnp.where(slot == ids, 1.0, 0.0).astype(bf16)
                rows = rows + jnp.dot(
                    hot,
                    total_s[at, lookup * row_width : (lookup + 1) * row_width],
                    preferred_element_type=f32,
                )

            @pl.when(i < dp_count)
            def _():
                send_s[b, j] = rows.astype(bf16)
                row_copy(b, j, i).start()

            @pl.when(i == dp_count)
            def _():
                got_s[b, me] = rows.astype(bf16)

            return carry

        lax.fori_loop(1 + part * dest_each, 1 + (part + 1) * dest_each, one, 0)

    row_tile = divisor(rows_dev, (256, 128))
    step_lanes = divisor(slots, (512, 384, 256, 128))

    table_steps = rows_dev // row_tile
    table_each = table_steps // 4 if table_steps % 4 == 0 else table_steps
    table_parts = table_steps // table_each

    def combine(b, part):
        def arrived(i, carry):
            row_copy(b, (me + i) % dp_count, i).wait_recv()
            return carry

        @pl.when(part == 0)
        def _():
            lax.fori_loop(1, dp_count, arrived, 0)

        def one(r, carry):
            at = pl.ds(pl.multiple_of(r * row_tile, row_tile), row_tile)
            row = lax.broadcasted_iota(jnp.int32, (row_tile, step_lanes), 0) + r * row_tile
            rows = got_s[b].reshape(slots, row_width)
            added = table_out[at, :]
            for start in range(0, slots, step_lanes):
                hot = jnp.where(row == gid_s[b, 0:1, start : start + step_lanes], 1.0, 0.0)
                added = added + jnp.dot(
                    hot.astype(bf16), rows[start : start + step_lanes], preferred_element_type=f32
                )
            table_out[at, :] = added
            return carry

        lax.fori_loop(part * table_each, (part + 1) * table_each, one, 0)

    wg_tile = divisor(mem, (128,))
    wg_steps = mem // wg_tile
    lag = 3
    late = lag + 2
    grads_every = 2
    ids_first = 4
    wg_first = grads_every * (tiles - 1) + 1
    pair_first = wg_first + wg_steps
    half_first = pair_first + 2
    half_every = 4
    dispatch_first = per_block + late
    combine_first = dispatch_first + dest_parts + 4
    total_steps = max(
        combine_first + (blocks - 1) * per_block + table_parts,
        half_first + half_every * bits + 1,
        chunks + late,
    )

    def every(s, first, period, count, then):
        at = s - first

        @pl.when(
            jnp.logical_and(at >= 0, jnp.logical_and(at % period == 0, at < count * period))
        )
        def _():
            then(at // period)

    def step(s, carry):
        every(s, 0, grads_every, tiles, grads)
        every(s, 1, grads_every * per_wide, wides - ahead, lambda i: project(i + ahead))

        @pl.when(jnp.logical_and(is_mid, s < chunks))
        def _():
            part_copy(s).wait_recv()
            at = chunk_at(s)
            part_s[at, :] = (part_s[at, :].astype(f32) + in_s[at, :].astype(f32)).astype(bf16)
            mid_copy(s).start()

        @pl.when(jnp.logical_and(is_mid, jnp.logical_and(s >= lag, s < chunks + lag)))
        def _():
            c = s - lag
            mid_copy(c).wait_recv()
            at = chunk_at(c)
            total_s[at, :] = (part_s[at, :].astype(f32) + mid_s[at, :].astype(f32)).astype(bf16)
            total_copy(c).start()

        @pl.when(jnp.logical_and(is_end, jnp.logical_and(s >= late, s < chunks + late)))
        def _():
            total_copy(s - late).wait_recv()

        @pl.when(s == ids_first - 1)
        def _():
            for i in range(1, dp_count):
                ids_copy(i).wait_recv()
            lax.fori_loop(0, dp_count, own_slots, 0)

        for part in range(id_parts):
            every(s, ids_first + part, id_parts, blocks, lambda b, part=part: own_ids(b, part))

        for i in range(wg_steps):

            @pl.when(s == wg_first + i)
            def _(i=i):
                weight_grad(i * wg_tile, wg_tile)

        @pl.when(s == pair_first)
        def _():
            for k in range(chips):
                pair_copy(k).start()

        @pl.when(s == half_first)
        def _():
            pair_sum()
            half_start(bits - 1)

        for s_bit in range(bits - 1, -1, -1):

            @pl.when(s == half_first + half_every * (bits - s_bit))
            def _(s_bit=s_bit):
                half_sum(s_bit)
                if s_bit:
                    half_start(s_bit - 1)

        def spread(first, parts, work):
            at = s - first

            @pl.when(
                jnp.logical_and(
                    at >= 0,
                    jnp.logical_and(at % per_block < parts, at < blocks * per_block),
                )
            )
            def _():
                work(at // per_block, at % per_block)

        spread(dispatch_first, dest_parts, dispatch)
        spread(combine_first, table_parts, combine)
        return carry

    lax.fori_loop(0, total_steps, step, 0)

    for k in range(1, chips):
        s = k.bit_length() - 1
        if k - (1 << s) or s == bits - 1:
            gather_copy(s, k - (1 << s)).wait_send()
        half_copy(s, k - (1 << s)).wait_send()
    for k in range(chips):
        across_copy(k).wait_send()
        pair_copy(k).wait_send()
    for i in range(1, dp_count):
        ids_copy(i).wait_send()
    for i in range(wides):
        for n in range(1, t_count):
            sums_copy(i, n).wait_send()

    def sent(c, carry):
        @pl.when(is_end)
        def _():
            part_copy(c).wait_send()

        @pl.when(is_mid)
        def _():
            mid_copy(c).wait_send()
            total_copy(c).wait_send()

        return carry

    lax.fori_loop(0, chunks, sent, 0)

    def rows_sent(n, carry):
        b = n // (dp_count - 1)
        i = n % (dp_count - 1) + 1
        row_copy(b, (me + i) % dp_count, i).wait_send()
        return carry

    lax.fori_loop(0, blocks * (dp_count - 1), rows_sent, 0)


def adam_kernel(
    grad_ref, table_ref, first_ref, second_ref, new_table, new_first, new_second
):
    table_grad = grad_ref[...]
    first = beta_one * first_ref[...] + (1.0 - beta_one) * table_grad
    second = beta_two * second_ref[...] + (1.0 - beta_two) * table_grad * table_grad
    root = jnp.sqrt(second * (1.0 / correct_two)) + adam_eps
    new_table[...] = table_ref[...] - (learn_rate / correct_one) * first / root
    new_first[...] = first
    new_second[...] = second


def body(
    memory,
    hidden,
    grad_out,
    key_weight,
    value_weight,
    row_ids,
    embed_table,
    first_moment,
    second_moment,
):
    dp_count = lax.axis_size("dp")
    t_count = lax.axis_size("tensor")
    tokens, mem = memory.shape
    width = hidden.shape[1]
    shard = key_weight.shape[0]
    rows_dev, row_width = embed_table.shape
    lookups = row_ids.shape[1]
    block = tokens // t_count
    entries = block * lookups
    owners = dp_count * t_count
    chips = dp_count // 2
    cap = -(-max(2, 3 * entries // owners) // 16) * 16
    tile = divisor(block, (128,))
    chunk = divisor(tile, (32,))
    wide = divisor(tokens, (256, 128))
    chunks = tokens // chunk
    aligned = shard % 16 == 0
    if t_count != 4 or chips & (chips - 1) or (dp_count * cap) % lanes:
        raise ValueError("unsupported mesh")
    plan = dict(
        dp=dp_count, tensor=t_count, tokens=tokens, mem=mem, width=width, shard=shard, cap=cap,
        rows_dev=rows_dev, lookups=lookups, row_width=row_width, block=block, tile=tile,
        chunk=chunk, aligned=aligned, wide=wide,
    )
    ids = row_ids.reshape(t_count, block, lookups).transpose(0, 2, 1).reshape(t_count, entries)
    dma = pltpu.SemaphoreType.DMA
    vmem = pltpu.VMEM
    hbm = pl.BlockSpec(memory_space=pltpu.HBM)
    inside = pl.BlockSpec(memory_space=pltpu.VMEM)
    slab_rows = (1, 16, lanes) if aligned else (dp_count, shard, 2 * width)
    key_grad, value_grad, table_grad = pl.pallas_call(
        lambda *refs: step_kernel(plan, *refs),
        in_specs=[hbm] * 6,
        out_specs=[inside] * 3,
        out_shape=[
            jax.ShapeDtypeStruct((shard, width), f32),
            jax.ShapeDtypeStruct((shard, width), f32),
            jax.ShapeDtypeStruct((rows_dev, row_width), f32),
        ],
        scratch_shapes=[
            vmem((tokens, mem), bf16),
            vmem((tokens, width), bf16),
            vmem((tokens, width), bf16),
            vmem((mem, 2 * width), bf16),
            vmem(slab_rows, bf16),
            vmem((tokens, width), f32),
            vmem((tokens, 2 * width), bf16),
            vmem((tokens, mem), bf16),
            vmem((tokens, mem), bf16),
            vmem((tokens, mem), bf16),
            vmem((tokens, mem), bf16),
            vmem((tokens // wide, t_count, sublanes, wide), f32),
            vmem((dp_count + 2, t_count, entries), jnp.int32),
            vmem((2 * sublanes, entries), jnp.int32),
            vmem((dp_count + 2, t_count, entries), jnp.int32),
            vmem((t_count, sublanes, dp_count * cap), jnp.int32),
            vmem((t_count, dp_count, cap, row_width), bf16),
            vmem((t_count, dp_count, cap, row_width), bf16),
            vmem((mem, 2 * width), bf16),
            vmem(slab_rows, bf16),
            vmem((chips, shard, 2 * width), bf16),
            vmem((chips, shard, 2 * width), bf16),
            dma((6,)),
            dma((dp_count,)),
            dma((dp_count,)),
            dma((chips,)),
            dma((chips,)),
            dma((chips,)),
            dma((chips,)),
            dma((tokens // wide, t_count)),
            dma((tokens // wide, t_count)),
            dma((chunks,)),
            dma((chunks,)),
            dma((chunks,)),
            dma((chunks,)),
            dma((chunks,)),
            dma((chunks,)),
            dma((t_count, dp_count)),
            dma((t_count, dp_count)),
            dma((chips,)),
            dma((chips,)),
            dma((chips,)),
            dma((chips,)),
        ],
        compiler_params=pltpu.CompilerParams(
            collective_id=0, has_side_effects=True, vmem_limit_bytes=67043328
        ),
        name="step",
    )(memory, hidden, grad_out, key_weight, value_weight, ids)
    row_tile = divisor(rows_dev, (512, 256, 128))
    row_spec = pl.BlockSpec((row_tile, row_width), lambda i: (i, 0))
    table_shape = jax.ShapeDtypeStruct((rows_dev, row_width), f32)
    new_table, new_first, new_second = pl.pallas_call(
        adam_kernel,
        grid=(rows_dev // row_tile,),
        in_specs=[row_spec] * 4,
        out_specs=[row_spec] * 3,
        out_shape=[table_shape] * 3,
        name="adam",
    )(table_grad, embed_table, first_moment, second_moment)
    return (key_grad, value_grad, new_table, new_first, new_second)


def solution(mesh):
    return jax.shard_map(
        body,
        mesh=mesh,
        in_specs=(
            P("dp", None),
            P("dp", "tensor"),
            P("dp", "tensor"),
            P("dp", "tensor"),
            P("dp", "tensor"),
            P("dp", None),
            P(("dp", "tensor"), None),
            P(("dp", "tensor"), None),
            P(("dp", "tensor"), None),
        ),
        out_specs=(
            P("dp", "tensor"),
            P("dp", "tensor"),
            P(("dp", "tensor"), None),
            P(("dp", "tensor"), None),
            P(("dp", "tensor"), None),
        ),
        check_vma=False,
    )
```

```python
import math

import jax
import jax.numpy as jnp
from jax import lax
from jax.experimental import pallas as pl
from jax.experimental.pallas import tpu as pltpu
from jax.sharding import PartitionSpec as P

beta_one = 0.9
beta_two = 0.999
learn_rate = 0.01
adam_eps = 1e-08
norm_eps = 1e-06
correct_one = 0.9999734386011124
correct_two = 0.0952078528863


f32 = jnp.float32
bf16 = jnp.bfloat16
lanes = 128
sublanes = 8


MESH = pl.DeviceIdType.MESH
contract_lanes = (((1,), (1,)), ((), ()))
contract_rows = (((0,), (0,)), ((), ()))


def divisor(count, choices):
    return next((c for c in choices if count % c == 0), count)


def step_kernel(
    plan,
    memory_hbm,
    hidden_hbm,
    grad_hbm,
    key_w_hbm,
    value_w_hbm,
    ids_hbm,
    key_out,
    value_out,
    table_out,
    mem_s,
    hid_s,
    grd_s,
    w_s,
    w_slab_s,
    key_s,
    both_s,
    part_s,
    in_s,
    mid_s,
    total_s,
    sums_s,
    ids_s,
    slot_s,
    own_s,
    gid_s,
    send_s,
    got_s,
    wg_s,
    wg_slab_s,
    pair_s,
    half_s,
    local_sem,
    ids_ssem,
    ids_rsem,
    ag_ssem,
    ag_rsem,
    dd_ssem,
    dd_rsem,
    sum_ssem,
    sum_rsem,
    part_ssem,
    part_rsem,
    mid_ssem,
    mid_rsem,
    total_ssem,
    total_rsem,
    row_ssem,
    row_rsem,
    pair_ssem,
    pair_rsem,
    half_ssem,
    half_rsem,
):
    dp_count, t_count = plan["dp"], plan["tensor"]
    tokens, mem, width = plan["tokens"], plan["mem"], plan["width"]
    shard, cap, rows_dev = plan["shard"], plan["cap"], plan["rows_dev"]
    lookups, row_width = plan["lookups"], plan["row_width"]
    blocks, block, tile, chunk = t_count, plan["block"], plan["tile"], plan["chunk"]
    aligned = plan["aligned"]
    model_width = width * t_count
    entries = block * lookups
    chips = dp_count // 2
    bits = chips.bit_length() - 1
    chunks = tokens // chunk
    tiles = tokens // tile
    per_tile = tile // chunk
    wide = plan["wide"]
    wides = tokens // wide
    per_wide = wide // tile
    per_block = block // chunk
    slots = dp_count * cap

    me = lax.axis_index("dp")
    z = lax.axis_index("tensor")
    core = me % 2
    chip = me // 2
    partner = chip * 2 + 1 - core
    is_mid = jnp.logical_and(z > 0, z < t_count - 1)
    is_end = jnp.logical_or(z == 0, z == t_count - 1)
    mate = z + 1 - 2 * (z % 2)
    other = t_count - 1 - z

    def remote(src, dst, ssem, rsem, dev_dp, dev_z):
        return pltpu.make_async_remote_copy(
            src_ref=src,
            dst_ref=dst,
            send_sem=ssem,
            recv_sem=rsem,
            device_id=(dev_dp, dev_z),
            device_id_type=MESH,
        )

    def slab_of(flat, stacked, index):
        if aligned:
            return flat.at[pl.ds(pl.multiple_of(index * shard, shard), shard)]
        return stacked.at[index]

    def w_slab(index):
        return slab_of(w_s, w_slab_s, index)

    def wg_slab(index):
        return slab_of(wg_s, wg_slab_s, index)

    own = w_slab(me)
    local = [
        pltpu.make_async_copy(key_w_hbm, own.at[:, :width], local_sem.at[0]),
        pltpu.make_async_copy(value_w_hbm, own.at[:, width:], local_sem.at[1]),
        pltpu.make_async_copy(ids_hbm, ids_s.at[me], local_sem.at[2]),
        pltpu.make_async_copy(memory_hbm, mem_s, local_sem.at[3]),
        pltpu.make_async_copy(hidden_hbm, hid_s, local_sem.at[4]),
        pltpu.make_async_copy(grad_hbm, grd_s, local_sem.at[5]),
    ]
    for copy in local:
        copy.start()

    barrier = pltpu.get_barrier_semaphore()
    for i in range(1, dp_count):
        pl.semaphore_signal(
            barrier, inc=1, device_id=((me + i) % dp_count, z), device_id_type=MESH
        )
    for i in range(1, t_count):
        pl.semaphore_signal(
            barrier, inc=1, device_id=(me, (z + i) % t_count), device_id_type=MESH
        )
    pl.semaphore_wait(barrier, dp_count - 1 + t_count - 1)

    def flip(x, s):
        a, b = 1 << s, 1 << (bits - 1 - s)
        f0 = x + a * (1 - 2 * ((x // a) % 2))
        f1 = x + b * (1 - 2 * ((x // b) % 2))
        return f0 * (1 - core) + f1 * core

    have = [chip]
    for s in range(bits):
        have = have + [flip(x, s) for x in have]

    def gather_copy(s, k):
        at = (1 << s) + k
        ref = w_slab(have[k] * 2 + core)
        return remote(ref, ref, ag_ssem.at[at], ag_rsem.at[at], flip(chip, s) * 2 + core, z)

    def across_copy(k):
        ref = w_slab(have[k] * 2 + core)
        return remote(ref, ref, dd_ssem.at[k], dd_rsem.at[k], partner, z)

    def ids_copy(i):
        ref = ids_s.at[me]
        return remote(ref, ref, ids_ssem.at[i], ids_rsem.at[i], (me + i) % dp_count, z)

    local[0].wait()
    local[1].wait()
    across_copy(0).start()
    for s in range(bits):
        if s:
            gather_copy(s - 1, 0).wait_send()
        gather_copy(s, 0).start()
    local[2].wait()

    upper = (
        lax.broadcasted_iota(jnp.int32, (lanes, lanes), 0)
        <= lax.broadcasted_iota(jnp.int32, (lanes, lanes), 1)
    )
    upper = jnp.where(upper, 1.0, 0.0).astype(bf16)

    def running(hits):
        carry = jnp.zeros((hits.shape[0], 1), f32)
        parts = []
        for start in range(0, entries, lanes):
            part = carry + jnp.dot(
                hits[:, start : start + lanes].astype(bf16), upper, preferred_element_type=f32
            )
            carry = part[:, lanes - 1 : lanes]
            parts.append(part)
        return jnp.concatenate(parts, axis=1)

    dest = lax.broadcasted_iota(jnp.int32, (dp_count, entries), 0)
    for b in range(blocks):
        owner_of = lax.div(ids_s[me, b : b + 1, :], jnp.int32(rows_dev))
        hits = jnp.where(owner_of == dest * t_count + z, 1.0, 0.0)
        ranked = hits * (running(hits) + (dest * cap).astype(f32))
        slot_s[b : b + 1, :] = jnp.sum(ranked, axis=0, keepdims=True).astype(jnp.int32) - 1

    def forward(k):
        s = k.bit_length() - 1
        gather_copy(s, k - (1 << s)).wait_recv()
        for later in range(s + 1, bits):
            gather_copy(later, k).start()
        across_copy(k).start()

    for k in range(1, chips):
        forward(k)
    for i in range(1, dp_count):
        ids_copy(i).start()

    def own_slots(j, carry):
        owner_of = lax.div(ids_s[j], jnp.int32(rows_dev))
        hits = jnp.where(owner_of == me * t_count + z, 1.0, 0.0)
        own_s[j] = (hits * running(hits)).astype(jnp.int32) - 1
        return carry

    id_tiles = slots // lanes
    id_parts = divisor(id_tiles, (4, 3, 2))
    id_each = id_tiles // id_parts

    def own_ids(b, part):
        for start in range(part * id_each * lanes, (part + 1) * id_each * lanes, lanes):
            first = start // cap
            last = (start + lanes - 1) // cap
            found = jnp.zeros((sublanes, lanes), f32)
            for j in range(first, last + 1):
                local_row = lax.rem(ids_s[j, pl.ds(b, 1), :], jnp.int32(rows_dev)) + 1
                row = lax.broadcasted_iota(jnp.int32, (sublanes, entries), 0)
                codes = jnp.where(
                    row == 0,
                    lax.div(local_row, jnp.int32(64)),
                    jnp.where(row == 1, lax.rem(local_row, jnp.int32(64)), 0),
                )
                slot = lax.broadcasted_iota(jnp.int32, (lanes, entries), 0) + (start - j * cap)
                hot = jnp.where(slot == own_s[j, pl.ds(b, 1), :], 1.0, 0.0)
                hot = jnp.where(slot < 0, 0.0, hot)
                found = found + lax.dot_general(
                    codes.astype(f32).astype(bf16),
                    hot.astype(bf16),
                    contract_lanes,
                    preferred_element_type=f32,
                )
            ids = found[0:1] * 64.0 + found[1:2] - 1.0
            gid_s[b, :, start : start + lanes] = jnp.broadcast_to(
                ids.astype(jnp.int32), (sublanes, lanes)
            )

    for k in range(chips):
        across_copy(k).wait_recv()
    if not aligned:
        for d in range(dp_count):
            w_s[d * shard : (d + 1) * shard, :] = w_slab_s[d]

    for copy in local[3:]:
        copy.wait()
    def project(i):
        at = pl.ds(pl.multiple_of(i * wide, wide), wide)
        proj = jnp.dot(mem_s[at, :], w_s[...], preferred_element_type=f32)
        key_proj = proj[:, :width]
        key_s[at, :] = key_proj
        square = jnp.sum(key_proj * key_proj, axis=1, keepdims=True)
        cross = jnp.sum(hid_s[at, :].astype(f32) * key_proj, axis=1, keepdims=True)
        output = jnp.sum(grd_s[at, :].astype(f32) * proj[:, width:], axis=1, keepdims=True)
        lane = lax.broadcasted_iota(jnp.int32, (wide, lanes), 1)
        packed = jnp.where(
            lane == 0, square, jnp.where(lane == 1, cross, jnp.where(lane == 2, output, 0.0))
        )
        sums_s[i, z] = packed.T[:sublanes, :]
        for n in range(1, t_count):
            sums_copy(i, n).start()

    def sums_copy(i, n):
        ref = sums_s.at[i, z]
        return remote(ref, ref, sum_ssem.at[i, n], sum_rsem.at[i, n], me, (z + n) % t_count)

    ahead = min(2, wides)
    for i in range(ahead):
        project(i)
    table_out[...] = jnp.zeros(table_out.shape, f32)

    def chunk_at(c):
        return pl.ds(pl.multiple_of(c * chunk, chunk), chunk)

    def part_copy(c):
        at = chunk_at(c)
        return remote(part_s.at[at], in_s.at[at], part_ssem.at[c], part_rsem.at[c], me, mate)

    def mid_copy(c):
        at = chunk_at(c)
        return remote(part_s.at[at], mid_s.at[at], mid_ssem.at[c], mid_rsem.at[c], me, other)

    def total_copy(c):
        at = chunk_at(c)
        return remote(total_s.at[at], total_s.at[at], total_ssem.at[c], total_rsem.at[c], me, mate)

    def grads(i):
        at = pl.ds(pl.multiple_of(i * tile, tile), tile)
        group = i // per_wide

        @pl.when(i % per_wide == 0)
        def _():
            for n in range(1, t_count):
                sums_copy(group, n).wait_recv()

        lane_at = pl.ds(pl.multiple_of((i % per_wide) * tile, tile), tile)
        sums = sums_s[group, 0, :, lane_at]
        for part in range(1, t_count):
            sums = sums + sums_s[group, part, :, lane_at]
        root_width = math.sqrt(model_width)
        key_scale = jnp.sqrt(sums[0:1] / model_width + norm_eps)
        gate_score = sums[1:2] / (key_scale * root_width)
        gate_value = 1.0 / (1.0 + jnp.exp(-gate_score))
        gate_grad = gate_value * (1.0 - gate_value) * sums[2:3]
        hidden_factor = gate_grad / (key_scale * root_width)
        key_factor = gate_grad * (gate_score / (model_width * key_scale * key_scale))
        row = lax.broadcasted_iota(jnp.int32, (lanes, tile), 0)
        factors = jnp.where(
            row == 0, hidden_factor, jnp.where(row == 1, key_factor, gate_value)
        ).T
        both_s[at, :width] = (
            factors[:, 0:1] * hid_s[at, :].astype(f32) - factors[:, 1:2] * key_s[at, :]
        ).astype(bf16)
        both_s[at, width:] = (factors[:, 2:3] * grd_s[at, :].astype(f32)).astype(bf16)
        part_s[at, :] = lax.dot_general(
            both_s[at, :], w_s[...], contract_lanes, preferred_element_type=f32
        ).astype(bf16)

        @pl.when(is_end)
        def _():
            for k in range(per_tile):
                part_copy(i * per_tile + k).start()

    def weight_grad(start, size):
        value = lax.dot_general(
            mem_s[:, start : start + size], both_s[...], contract_rows, preferred_element_type=f32
        ).astype(bf16)
        if aligned:
            wg_s[start : start + size, :] = value
        else:
            at = start
            while at < start + size:
                d = at // shard
                stop = min((d + 1) * shard, start + size)
                wg_slab_s[d, at - d * shard : stop - d * shard, :] = value[
                    at - start : stop - start
                ]
                at = stop

    def pair_copy(k):
        return remote(
            wg_slab(k * 2 + 1 - core), pair_s.at[k], pair_ssem.at[k], pair_rsem.at[k], partner, z
        )

    def half_copy(s, k):
        at = (1 << s) + k
        return remote(
            wg_slab(have[at] * 2 + core),
            half_s.at[at],
            half_ssem.at[at],
            half_rsem.at[at],
            flip(chip, s) * 2 + core,
            z,
        )

    def half_start(s):
        for k in range(1 << s):
            half_copy(s, k).start()

    def pair_sum():
        for k in range(chips):
            pair_copy(k).wait_recv()
        for k in range(chips):
            ref = wg_slab(k * 2 + core)
            ref[...] = (ref[...].astype(f32) + pair_s[k].astype(f32)).astype(bf16)

    def half_sum(s):
        for k in range(1 << s):
            half_copy(s, k).wait_recv()
        for k in range(1 << s):
            ref = wg_slab(have[k] * 2 + core)
            added = ref[...].astype(f32) + half_s[(1 << s) + k].astype(f32)
            if s:
                ref[...] = added.astype(bf16)
            else:
                key_out[...] = added[:, :width]
                value_out[...] = added[:, width:]

    def row_copy(b, j, i):
        return remote(
            send_s.at[b, j], got_s.at[b, me], row_ssem.at[b, i], row_rsem.at[b, i], j, z
        )

    dest_each = dp_count // 4 if dp_count % 4 == 0 else dp_count
    dest_parts = dp_count // dest_each

    def dispatch(b, part):
        def one(i, carry):
            j = (me + i) % dp_count
            slot = lax.broadcasted_iota(jnp.int32, (cap, block), 0) + j * cap
            rows = jnp.zeros((cap, row_width), f32)
            at = pl.ds(pl.multiple_of(b * block, block), block)
            for lookup in range(lookups):
                ids = slot_s[pl.ds(b, 1), lookup * block : (lookup + 1) * block]
                hot = jnp.where(slot == ids, 1.0, 0.0).astype(bf16)
                rows = rows + jnp.dot(
                    hot,
                    total_s[at, lookup * row_width : (lookup + 1) * row_width],
                    preferred_element_type=f32,
                )

            @pl.when(i < dp_count)
            def _():
                send_s[b, j] = rows.astype(bf16)
                row_copy(b, j, i).start()

            @pl.when(i == dp_count)
            def _():
                got_s[b, me] = rows.astype(bf16)

            return carry

        lax.fori_loop(1 + part * dest_each, 1 + (part + 1) * dest_each, one, 0)

    row_tile = divisor(rows_dev, (256, 128))
    step_lanes = divisor(slots, (512, 384, 256, 128))

    table_steps = rows_dev // row_tile
    table_each = table_steps // 4 if table_steps % 4 == 0 else table_steps
    table_parts = table_steps // table_each

    def combine(b, part):
        def arrived(i, carry):
            row_copy(b, (me + i) % dp_count, i).wait_recv()
            return carry

        @pl.when(part == 0)
        def _():
            lax.fori_loop(1, dp_count, arrived, 0)

        def one(r, carry):
            at = pl.ds(pl.multiple_of(r * row_tile, row_tile), row_tile)
            row = lax.broadcasted_iota(jnp.int32, (row_tile, step_lanes), 0) + r * row_tile
            rows = got_s[b].reshape(slots, row_width)
            added = table_out[at, :]
            for start in range(0, slots, step_lanes):
                hot = jnp.where(row == gid_s[b, 0:1, start : start + step_lanes], 1.0, 0.0)
                added = added + jnp.dot(
                    hot.astype(bf16), rows[start : start + step_lanes], preferred_element_type=f32
                )
            table_out[at, :] = added
            return carry

        lax.fori_loop(part * table_each, (part + 1) * table_each, one, 0)

    wg_tile = divisor(mem, (128,))
    wg_steps = mem // wg_tile
    lag = 4
    late = lag + 2
    grads_every = 3
    ids_first = 4
    wg_first = grads_every * (tiles - 1) + 1
    pair_first = wg_first + wg_steps
    half_first = pair_first + 2
    half_every = 7
    dispatch_first = per_block + late
    combine_first = dispatch_first + dest_parts + 4
    total_steps = max(
        combine_first + (blocks - 1) * per_block + table_parts,
        half_first + half_every * bits + 1,
        chunks + late,
    )

    def every(s, first, period, count, then):
        at = s - first

        @pl.when(
            jnp.logical_and(at >= 0, jnp.logical_and(at % period == 0, at < count * period))
        )
        def _():
            then(at // period)

    def step(s, carry):
        every(s, 0, grads_every, tiles, grads)
        every(s, 1, grads_every * per_wide, wides - ahead, lambda i: project(i + ahead))

        @pl.when(jnp.logical_and(is_mid, s < chunks))
        def _():
            part_copy(s).wait_recv()
            at = chunk_at(s)
            part_s[at, :] = (part_s[at, :].astype(f32) + in_s[at, :].astype(f32)).astype(bf16)
            mid_copy(s).start()

        @pl.when(jnp.logical_and(is_mid, jnp.logical_and(s >= lag, s < chunks + lag)))
        def _():
            c = s - lag
            mid_copy(c).wait_recv()
            at = chunk_at(c)
            total_s[at, :] = (part_s[at, :].astype(f32) + mid_s[at, :].astype(f32)).astype(bf16)
            total_copy(c).start()

        @pl.when(jnp.logical_and(is_end, jnp.logical_and(s >= late, s < chunks + late)))
        def _():
            total_copy(s - late).wait_recv()

        @pl.when(s == ids_first - 1)
        def _():
            for i in range(1, dp_count):
                ids_copy(i).wait_recv()
            lax.fori_loop(0, dp_count, own_slots, 0)

        for part in range(id_parts):
            every(s, ids_first + part, id_parts, blocks, lambda b, part=part: own_ids(b, part))

        for i in range(wg_steps):

            @pl.when(s == wg_first + i)
            def _(i=i):
                weight_grad(i * wg_tile, wg_tile)

        @pl.when(s == pair_first)
        def _():
            for k in range(chips):
                pair_copy(k).start()

        @pl.when(s == half_first)
        def _():
            pair_sum()
            half_start(bits - 1)

        for s_bit in range(bits - 1, -1, -1):

            @pl.when(s == half_first + half_every * (bits - s_bit))
            def _(s_bit=s_bit):
                half_sum(s_bit)
                if s_bit:
                    half_start(s_bit - 1)

        def spread(first, parts, work):
            at = s - first

            @pl.when(
                jnp.logical_and(
                    at >= 0,
                    jnp.logical_and(at % per_block < parts, at < blocks * per_block),
                )
            )
            def _():
                work(at // per_block, at % per_block)

        spread(dispatch_first, dest_parts, dispatch)
        spread(combine_first, table_parts, combine)
        return carry

    lax.fori_loop(0, total_steps, step, 0)

    for k in range(1, chips):
        s = k.bit_length() - 1
        if k - (1 << s) or s == bits - 1:
            gather_copy(s, k - (1 << s)).wait_send()
        half_copy(s, k - (1 << s)).wait_send()
    for k in range(chips):
        across_copy(k).wait_send()
        pair_copy(k).wait_send()
    for i in range(1, dp_count):
        ids_copy(i).wait_send()
    for i in range(wides):
        for n in range(1, t_count):
            sums_copy(i, n).wait_send()

    def sent(c, carry):
        @pl.when(is_end)
        def _():
            part_copy(c).wait_send()

        @pl.when(is_mid)
        def _():
            mid_copy(c).wait_send()
            total_copy(c).wait_send()

        return carry

    lax.fori_loop(0, chunks, sent, 0)

    def rows_sent(n, carry):
        b = n // (dp_count - 1)
        i = n % (dp_count - 1) + 1
        row_copy(b, (me + i) % dp_count, i).wait_send()
        return carry

    lax.fori_loop(0, blocks * (dp_count - 1), rows_sent, 0)


def adam_kernel(
    grad_ref, table_ref, first_ref, second_ref, new_table, new_first, new_second
):
    table_grad = grad_ref[...]
    first = beta_one * first_ref[...] + (1.0 - beta_one) * table_grad
    second = beta_two * second_ref[...] + (1.0 - beta_two) * table_grad * table_grad
    root = jnp.sqrt(second * (1.0 / correct_two)) + adam_eps
    new_table[...] = table_ref[...] - (learn_rate / correct_one) * first / root
    new_first[...] = first
    new_second[...] = second


def body(
    memory,
    hidden,
    grad_out,
    key_weight,
    value_weight,
    row_ids,
    embed_table,
    first_moment,
    second_moment,
):
    dp_count = lax.axis_size("dp")
    t_count = lax.axis_size("tensor")
    tokens, mem = memory.shape
    width = hidden.shape[1]
    shard = key_weight.shape[0]
    rows_dev, row_width = embed_table.shape
    lookups = row_ids.shape[1]
    block = tokens // t_count
    entries = block * lookups
    owners = dp_count * t_count
    chips = dp_count // 2
    cap = -(-max(2, 3 * entries // owners) // 16) * 16
    tile = divisor(block, (128,))
    chunk = divisor(tile, (32,))
    wide = divisor(tokens, (256, 128))
    chunks = tokens // chunk
    aligned = shard % 16 == 0
    if t_count != 4 or chips & (chips - 1) or (dp_count * cap) % lanes:
        raise ValueError("unsupported mesh")
    plan = dict(
        dp=dp_count, tensor=t_count, tokens=tokens, mem=mem, width=width, shard=shard, cap=cap,
        rows_dev=rows_dev, lookups=lookups, row_width=row_width, block=block, tile=tile,
        chunk=chunk, aligned=aligned, wide=wide,
    )
    ids = row_ids.reshape(t_count, block, lookups).transpose(0, 2, 1).reshape(t_count, entries)
    dma = pltpu.SemaphoreType.DMA
    vmem = pltpu.VMEM
    hbm = pl.BlockSpec(memory_space=pltpu.HBM)
    inside = pl.BlockSpec(memory_space=pltpu.VMEM)
    slab_rows = (1, 16, lanes) if aligned else (dp_count, shard, 2 * width)
    key_grad, value_grad, table_grad = pl.pallas_call(
        lambda *refs: step_kernel(plan, *refs),
        in_specs=[hbm] * 6,
        out_specs=[inside] * 3,
        out_shape=[
            jax.ShapeDtypeStruct((shard, width), f32),
            jax.ShapeDtypeStruct((shard, width), f32),
            jax.ShapeDtypeStruct((rows_dev, row_width), f32),
        ],
        scratch_shapes=[
            vmem((tokens, mem), bf16),
            vmem((tokens, width), bf16),
            vmem((tokens, width), bf16),
            vmem((mem, 2 * width), bf16),
            vmem(slab_rows, bf16),
            vmem((tokens, width), f32),
            vmem((tokens, 2 * width), bf16),
            vmem((tokens, mem), bf16),
            vmem((tokens, mem), bf16),
            vmem((tokens, mem), bf16),
            vmem((tokens, mem), bf16),
            vmem((tokens // wide, t_count, sublanes, wide), f32),
            vmem((dp_count + 2, t_count, entries), jnp.int32),
            vmem((2 * sublanes, entries), jnp.int32),
            vmem((dp_count + 2, t_count, entries), jnp.int32),
            vmem((t_count, sublanes, dp_count * cap), jnp.int32),
            vmem((t_count, dp_count, cap, row_width), bf16),
            vmem((t_count, dp_count, cap, row_width), bf16),
            vmem((mem, 2 * width), bf16),
            vmem(slab_rows, bf16),
            vmem((chips, shard, 2 * width), bf16),
            vmem((chips, shard, 2 * width), bf16),
            dma((6,)),
            dma((dp_count,)),
            dma((dp_count,)),
            dma((chips,)),
            dma((chips,)),
            dma((chips,)),
            dma((chips,)),
            dma((tokens // wide, t_count)),
            dma((tokens // wide, t_count)),
            dma((chunks,)),
            dma((chunks,)),
            dma((chunks,)),
            dma((chunks,)),
            dma((chunks,)),
            dma((chunks,)),
            dma((t_count, dp_count)),
            dma((t_count, dp_count)),
            dma((chips,)),
            dma((chips,)),
            dma((chips,)),
            dma((chips,)),
        ],
        compiler_params=pltpu.CompilerParams(
            collective_id=0, has_side_effects=True, vmem_limit_bytes=67043328
        ),
        name="step",
    )(memory, hidden, grad_out, key_weight, value_weight, ids)
    row_tile = divisor(rows_dev, (512, 256, 128))
    row_spec = pl.BlockSpec((row_tile, row_width), lambda i: (i, 0))
    table_shape = jax.ShapeDtypeStruct((rows_dev, row_width), f32)
    new_table, new_first, new_second = pl.pallas_call(
        adam_kernel,
        grid=(rows_dev // row_tile,),
        in_specs=[row_spec] * 4,
        out_specs=[row_spec] * 3,
        out_shape=[table_shape] * 3,
        name="adam",
    )(table_grad, embed_table, first_moment, second_moment)
    return (key_grad, value_grad, new_table, new_first, new_second)


def solution(mesh):
    return jax.shard_map(
        body,
        mesh=mesh,
        in_specs=(
            P("dp", None),
            P("dp", "tensor"),
            P("dp", "tensor"),
            P("dp", "tensor"),
            P("dp", "tensor"),
            P("dp", None),
            P(("dp", "tensor"), None),
            P(("dp", "tensor"), None),
            P(("dp", "tensor"), None),
        ),
        out_specs=(
            P("dp", "tensor"),
            P("dp", "tensor"),
            P(("dp", "tensor"), None),
            P(("dp", "tensor"), None),
            P(("dp", "tensor"), None),
        ),
        check_vma=False,
    )
```
